32 devices in a mesh: dp: 2 (over z, core), tp: 16 (over x, y).
Axes of the slice: x: 4, y: 4, z: 1, core: 2. Of those that a mesh axis runs over, the one named last changes fastest.
The devices are a block of a 4x4x8 slice.
Arguments:
- x: bfloat16 [4096, 3584], P('dp'), parts along dimension 0
- dy: bfloat16 [4096, 3584], P('dp'), parts along dimension 0
- gate: bfloat16 [4096, 14336], P('dp', 'tp'), parts along dimension 0
- up: bfloat16 [4096, 14336], P('dp', 'tp'), parts along dimension 0
- w_gate: bfloat16 [3584, 14336], P(None, 'tp')
- w_up: bfloat16 [3584, 14336], P(None, 'tp')
- w_down: bfloat16 [14336, 3584], P('tp')
Outputs:
- output 1: bfloat16 [4096, 3584], P('dp'), parts along dimension 0
- output 2: bfloat16 [7168, 14336], P('dp', 'tp'), parts along dimension 0
- output 3: bfloat16 [7168, 14336], P('dp', 'tp'), parts along dimension 0
- output 4: bfloat16 [28672, 3584], P(('dp', 'tp')), parts along dimension 0
There are 2 independent parts. The reference program is written for one: setup_inputs(seed, part) draws one part's arguments, and reference() takes and returns one part's arrays. A program takes and returns all parts, laid end to end along the dimension named above; an argument that names none is the same for every part.
All inputs are finite; a program needn't handle non-finite values.
Results may differ from the reference program's by a relative error of at most 0.012.
Values are sent between devices in bfloat16 or wider.
A program may use at most 768 MiB of HBM per device.

```python
import jax
import jax.numpy as jnp

ROWS = 2048
D = 3584
FF = 14336


def act(gate, up):
    return jax.nn.gelu(gate) * up


def setup_inputs(seed: int = 0, part: int = 0) -> dict:
    kx, ky, ka, kb, kg, ku, kd = jax.random.split(jax.random.key(seed), 7)
    kx, ky, ka, kb = (jax.random.fold_in(k, part) for k in (kx, ky, ka, kb))
    drawn = {
        "x": jax.random.normal(kx, (ROWS, D), jnp.float32),
        "dy": jax.random.normal(ky, (ROWS, D), jnp.float32),
        "gate": jax.random.normal(ka, (ROWS, FF), jnp.float32),
        "up": jax.random.normal(kb, (ROWS, FF), jnp.float32),
        "w_gate": jax.random.normal(kg, (D, FF), jnp.float32) * D**-0.5,
        "w_up": jax.random.normal(ku, (D, FF), jnp.float32) * D**-0.5,
        "w_down": jax.random.normal(kd, (FF, D), jnp.float32) * FF**-0.5,
    }
    return {k: v.astype(jnp.bfloat16) for k, v in drawn.items()}


def reference(x, dy, gate, up, w_gate, w_up, w_down):
    hidden, back = jax.vjp(act, gate.astype(jnp.float32), up.astype(jnp.float32))
    d_hidden = jnp.dot(dy, w_down.T, preferred_element_type=jnp.float32)
    d_gate, d_up = (g.astype(jnp.bfloat16) for g in back(d_hidden))
    dx = jnp.dot(d_gate, w_gate.T, preferred_element_type=jnp.float32) + jnp.dot(d_up, w_up.T, preferred_element_type=jnp.float32)
    dw_gate = jnp.dot(x.T, d_gate, preferred_element_type=jnp.float32)
    dw_up = jnp.dot(x.T, d_up, preferred_element_type=jnp.float32)
    dw_down = jnp.dot(hidden.astype(jnp.bfloat16).T, dy, preferred_element_type=jnp.float32)
    return tuple(g.astype(jnp.bfloat16) for g in (dx, dw_gate, dw_up, dw_down))
```

```python
import functools
import math

import jax
import jax.numpy as jnp
from jax import lax
from jax.experimental import pallas as pl
from jax.experimental.pallas import tpu as pltpu
from jax.sharding import PartitionSpec as P

MESH = pl.DeviceIdType.MESH
F32 = jnp.float32
BF16 = jnp.bfloat16
LAST = (((1,), (1,)), ((), ()))

BLOCK = 256
SLAB = 256
ACT_ROWS = 32
HOPS = 3


def act(gate, up):
    return jax.nn.gelu(gate) * up


def kernel(
    side, x, dy, gate, up, w_gate, w_up, w_down,
    dx, dw_gate, dw_up, dw_down,
    wgu, wd, dgu, hid_t, dyb, gb, ub, dh, hb, term, acc, st1, rv1, st2, rv2, fin,
    xb, xt, yb, og, ou, od,
    in_sem, w_sem, s1_send, s2_send, r1_recv, r2_recv, ag_send, ag_recv, fin_sem,
    xy_sem, o_sem,
):
    rows, d = dx.shape
    ff = w_down.shape[0]
    blocks = rows // BLOCK
    part = BLOCK // side
    sub = part // side
    quarter = d // 4
    slabs = d // SLAB

    me = lax.axis_index("tp")
    px, py = me // side, me % side

    def device(axis, sign):
        if axis == 0:
            return {"tp": (px + side + sign) % side * side + py}
        return {"tp": px * side + (py + side + sign) % side}

    flows = ((0, 1, 1), (0, 1, -1), (1, 0, 1), (1, 0, -1))
    pos = (px, py)

    def cols(c):
        return pl.ds(c * quarter, quarter)

    def load_block(t, slot):
        r = pl.ds(pl.multiple_of(t * BLOCK, BLOCK), BLOCK)
        return (
            pltpu.make_async_copy(dy.at[r, :], dyb.at[slot], in_sem.at[slot, 0]),
            pltpu.make_async_copy(gate.at[r, :], gb.at[slot], in_sem.at[slot, 1]),
            pltpu.make_async_copy(up.at[r, :], ub.at[slot], in_sem.at[slot, 2]),
        )

    load_wd = pltpu.make_async_copy(w_down, wd, w_sem.at[0])
    load_wg = pltpu.make_async_copy(w_gate, wgu.at[:, pl.ds(0, ff)], w_sem.at[1])
    load_wu = pltpu.make_async_copy(w_up, wgu.at[:, pl.ds(ff, ff)], w_sem.at[2])

    load_wd.start()
    for copy in load_block(0, 0):
        copy.start()
    load_wg.start()
    load_wu.start()

    barrier = pltpu.get_barrier_semaphore()
    for axis in (0, 1):
        for sign in (1, -1):
            pl.semaphore_signal(barrier, inc=1, device_id=device(axis, sign), device_id_type=MESH)
    pl.semaphore_wait(barrier, 4)

    def hop(h, c, b):
        a1, a2, sign = flows[c]
        slot = b % 2
        if h < HOPS:
            return pltpu.make_async_remote_copy(
                st1.at[h, c], rv1.at[slot, h, c], s1_send.at[h, c], r1_recv.at[slot, h, c],
                device_id=device(a1, sign), device_id_type=MESH,
            )
        if h < 2 * HOPS:
            s = h - HOPS
            return pltpu.make_async_remote_copy(
                st2.at[s, c], rv2.at[slot, s, c], s2_send.at[s, c], r2_recv.at[slot, s, c],
                device_id=device(a2, sign), device_id_type=MESH,
            )
        s = h - 2 * HOPS
        p1, p2 = pos[a1], pos[a2]
        if s < HOPS:
            q = (p2 + side - sign * s) % side
            r = pl.ds(pl.multiple_of(b * BLOCK + p1 * part + q * sub, sub), sub)
            to = device(a2, sign)
        else:
            q = (p1 + side - sign * (s - HOPS)) % side
            r = pl.ds(pl.multiple_of(b * BLOCK + q * part, part), part)
            to = device(a1, sign)
        where = dx.at[r, cols(c)]
        return pltpu.make_async_remote_copy(
            fin.at[c] if s == 0 else where, where, ag_send.at[s, c], ag_recv.at[slot, s, c],
            device_id=to, device_id_type=MESH,
        )

    def own_piece(c, b):
        a1, a2, sign = flows[c]
        r = pl.ds(pl.multiple_of(b * BLOCK + pos[a1] * part + pos[a2] * sub, sub), sub)
        return pltpu.make_async_copy(fin.at[c], dx.at[r, cols(c)], fin_sem.at[c])

    def term_part(b, c, q):
        r = pl.ds(pl.multiple_of(q * part, part), part)
        return term[b % 3, r, cols(c)]

    def stage(h, b):
        for c in range(4):
            a1, a2, sign = flows[c]
            p1, p2 = pos[a1], pos[a2]
            if h > 0:
                hop(h - 1, c, b).wait_recv()
            if h < HOPS:
                q = (p1 + 2 * side - sign * (1 + h)) % side
                value = term_part(b, c, q)
                if h > 0:
                    value = value + rv1[b % 2, h - 1, c].astype(F32)
                st1[h, c] = value.astype(BF16)
            elif h < 2 * HOPS:
                s = h - HOPS
                if s == 0:
                    acc[b % 3, c] = term_part(b, c, p1) + rv1[b % 2, HOPS - 1, c].astype(F32)
                q = (p2 + 2 * side - sign * (1 + s)) % side
                value = acc[b % 3, c, pl.ds(pl.multiple_of(q * sub, sub), sub), :]
                if s > 0:
                    value = value + rv2[b % 2, s - 1, c].astype(F32)
                st2[s, c] = value.astype(BF16)
            elif h == 2 * HOPS:
                value = acc[b % 3, c, pl.ds(pl.multiple_of(p2 * sub, sub), sub), :]
                fin[c] = (value + rv2[b % 2, HOPS - 1, c].astype(F32)).astype(BF16)
                own_piece(c, b).start()
            elif h == 2 * HOPS + 1:
                own_piece(c, b).wait()
            if h < 4 * HOPS:
                hop(h, c, b).start()

    def compute(t):
        slot = t % 2
        for copy in load_block(t, slot):
            copy.wait()

        @pl.when(t + 1 < blocks)
        def _():
            for copy in load_block(t + 1, 1 - slot):
                copy.start()

        @pl.when(t == 0)
        def _():
            load_wd.wait()

        dh[...] = lax.dot_general(dyb[slot], wd[...], LAST, preferred_element_type=F32)
        base = pl.multiple_of(t * BLOCK, BLOCK)

        @pl.loop(0, BLOCK // ACT_ROWS)
        def _(i):
            r = pl.ds(pl.multiple_of(i * ACT_ROWS, ACT_ROWS), ACT_ROWS)
            g = pl.ds(pl.multiple_of(base + i * ACT_ROWS, ACT_ROWS), ACT_ROWS)
            hidden, back = jax.vjp(act, gb[slot, r, :].astype(F32), ub[slot, r, :].astype(F32))
            d_gate, d_up = back(dh[r, :])
            dgu[g, pl.ds(0, ff)] = d_gate.astype(BF16)
            dgu[g, pl.ds(ff, ff)] = d_up.astype(BF16)
            hb[r, :] = hidden.astype(BF16)

        hid_t[:, pl.ds(base, BLOCK)] = hb[...].T

        @pl.when(t == 0)
        def _():
            load_wg.wait()
            load_wu.wait()

        lhs = dgu[pl.ds(base, BLOCK), :]
        wide = d // 7

        @pl.loop(0, 7)
        def _(i):
            n = pl.ds(pl.multiple_of(i * wide, wide), wide)
            term[t % 3, :, n] = lax.dot_general(lhs, wgu[n, :], LAST, preferred_element_type=F32)

    def load_slab(j, slot):
        n = pl.ds(pl.multiple_of(j * SLAB, SLAB), SLAB)
        return (
            pltpu.make_async_copy(x.at[:, n], xb.at[slot], xy_sem.at[slot, 0]),
            pltpu.make_async_copy(dy.at[:, n], yb.at[slot], xy_sem.at[slot, 1]),
        )

    def store_slab(j, slot):
        n = pl.ds(pl.multiple_of(j * SLAB, SLAB), SLAB)
        return (
            pltpu.make_async_copy(og.at[slot], dw_gate.at[n, :], o_sem.at[slot, 0]),
            pltpu.make_async_copy(ou.at[slot], dw_up.at[n, :], o_sem.at[slot, 1]),
            pltpu.make_async_copy(od.at[slot], dw_down.at[:, n], o_sem.at[slot, 2]),
        )

    def weights(j):
        slot = j % 2
        for copy in load_slab(j, slot):
            copy.wait()

        @pl.when(j >= 2)
        def _():
            for copy in store_slab(j - 2, slot):
                copy.wait()

        xt[...] = xb[slot].T
        og[slot] = jnp.dot(xt[...], dgu[:, pl.ds(0, ff)], preferred_element_type=F32).astype(BF16)
        ou[slot] = jnp.dot(xt[...], dgu[:, pl.ds(ff, ff)], preferred_element_type=F32).astype(BF16)
        od[slot] = jnp.dot(hid_t[...], yb[slot], preferred_element_type=F32).astype(BF16)
        for copy in store_slab(j, slot):
            copy.start()

        @pl.when(j + 2 < slabs)
        def _():
            for copy in load_slab(j + 2, slot):
                copy.start()

    @pl.loop(0, blocks + 4 * HOPS + 1)
    def _(t):
        for h in range(4 * HOPS, 0, -1):
            b = t - h
            if h < 4 * HOPS:
                @pl.when((b >= 1) & (b <= blocks))
                def _():
                    for c in range(4):
                        hop(h, c, b - 1).wait_send()

            @pl.when((b >= 0) & (b < blocks))
            def _():
                stage(h, b)

        @pl.when((t >= 1) & (t <= blocks))
        def _():
            for c in range(4):
                hop(0, c, t - 1).wait_send()

        @pl.when(t < blocks)
        def _():
            compute(t)
            stage(0, t)

        @pl.when(t == blocks - 1)
        def _():
            for j in range(2):
                for copy in load_slab(j, j):
                    copy.start()

        first = (t - blocks) * 2

        @pl.when((t >= blocks) & (first < slabs))
        def _():
            @pl.loop(0, 2)
            def _(i):
                weights(first + i)

    for j in range(slabs - 2, slabs):
        for copy in store_slab(j, j % 2):
            copy.wait()


def solution(mesh):
    n = mesh.shape["tp"]
    side = math.isqrt(n)

    def step(x, dy, gate, up, w_gate, w_up, w_down):
        rows, d = x.shape
        ff = w_down.shape[0]
        part = BLOCK // side
        sub = part // side
        quarter = d // 4
        hbm = pl.BlockSpec(memory_space=pl.ANY)
        dma = pltpu.SemaphoreType.DMA
        return pl.pallas_call(
            functools.partial(kernel, side),
            out_shape=(
                jax.ShapeDtypeStruct((rows, d), BF16),
                jax.ShapeDtypeStruct((d, ff), BF16),
                jax.ShapeDtypeStruct((d, ff), BF16),
                jax.ShapeDtypeStruct((ff, d), BF16),
            ),
            in_specs=[hbm] * 7,
            out_specs=(hbm,) * 4,
            scratch_shapes=[
                pltpu.VMEM((d, 2 * ff), BF16),
                pltpu.VMEM((ff, d), BF16),
                pltpu.VMEM((rows, 2 * ff), BF16),
                pltpu.VMEM((ff, rows), BF16),
                pltpu.VMEM((2, BLOCK, d), BF16),
                pltpu.VMEM((2, BLOCK, ff), BF16),
                pltpu.VMEM((2, BLOCK, ff), BF16),
                pltpu.VMEM((BLOCK, ff), F32),
                pltpu.VMEM((BLOCK, ff), BF16),
                pltpu.VMEM((3, BLOCK, d), F32),
                pltpu.VMEM((3, 4, part, quarter), F32),
                pltpu.VMEM((HOPS, 4, part, quarter), BF16),
                pltpu.VMEM((2, HOPS, 4, part, quarter), BF16),
                pltpu.VMEM((HOPS, 4, sub, quarter), BF16),
                pltpu.VMEM((2, HOPS, 4, sub, quarter), BF16),
                pltpu.VMEM((4, sub, quarter), BF16),
                pltpu.VMEM((2, rows, SLAB), BF16),
                pltpu.VMEM((SLAB, rows), BF16),
                pltpu.VMEM((2, rows, SLAB), BF16),
                pltpu.VMEM((2, SLAB, ff), BF16),
                pltpu.VMEM((2, SLAB, ff), BF16),
                pltpu.VMEM((2, ff, SLAB), BF16),
                dma((2, 3)),
                dma((3,)),
                dma((HOPS, 4)),
                dma((HOPS, 4)),
                dma((2, HOPS, 4)),
                dma((2, HOPS, 4)),
                dma((2 * HOPS, 4)),
                dma((2, 2 * HOPS, 4)),
                dma((4,)),
                dma((2, 2)),
                dma((2, 3)),
            ],
            compiler_params=pltpu.CompilerParams(
                collective_id=0, has_side_effects=True, vmem_limit_bytes=67043328
            ),
        )(x, dy, gate, up, w_gate, w_up, w_down)

    tokens, columns, rows = P("dp", None), P(None, "tp"), P("tp", None)
    return jax.shard_map(
        step,
        mesh=mesh,
        in_specs=(tokens, tokens, P("dp", "tp"), P("dp", "tp"), columns, columns, rows),
        out_specs=(tokens, P("dp", "tp"), P("dp", "tp"), P(("dp", "tp"), None)),
        check_vma=False,
    )
```

```python
import functools
import math

import jax
import jax.numpy as jnp
from jax import lax
from jax.experimental import pallas as pl
from jax.experimental.pallas import tpu as pltpu
from jax.sharding import PartitionSpec as P

MESH = pl.DeviceIdType.MESH
F32 = jnp.float32
BF16 = jnp.bfloat16
LAST = (((1,), (1,)), ((), ()))

BLOCK = 256
SLAB = 256
ACT_ROWS = 32
HOPS = 3


def act(gate, up):
    return jax.nn.gelu(gate) * up


def kernel(
    side, x, dy, gate, up, w_gate, w_up, w_down,
    dx, wgu, wd,
    dgu, hid_t, dyb, gb, ub, dh, hb, term, acc, st1, rv1, st2, rv2, fin, xb, xt, yb,
    in_sem, w_sem, s1_send, s2_send, r1_recv, r2_recv, ag_send, ag_recv, fin_sem, xy_sem,
):
    rows, d = dx.shape
    ff = w_down.shape[0]
    blocks = rows // BLOCK
    part = BLOCK // side
    sub = part // side
    quarter = d // 4
    slabs = d // SLAB

    me = lax.axis_index("tp")
    px, py = me // side, me % side

    def device(axis, sign):
        if axis == 0:
            return {"tp": (px + side + sign) % side * side + py}
        return {"tp": px * side + (py + side + sign) % side}

    flows = ((0, 1, 1), (0, 1, -1), (1, 0, 1), (1, 0, -1))
    pos = (px, py)

    def cols(c):
        return pl.ds(c * quarter, quarter)

    def load_block(t, slot):
        r = pl.ds(pl.multiple_of(t * BLOCK, BLOCK), BLOCK)
        return (
            pltpu.make_async_copy(dy.at[r, :], dyb.at[slot], in_sem.at[slot, 0]),
            pltpu.make_async_copy(gate.at[r, :], gb.at[slot], in_sem.at[slot, 1]),
            pltpu.make_async_copy(up.at[r, :], ub.at[slot], in_sem.at[slot, 2]),
        )

    load_wd = pltpu.make_async_copy(w_down, wd, w_sem.at[0])
    load_wg = pltpu.make_async_copy(w_gate, wgu.at[:, pl.ds(0, ff)], w_sem.at[1])
    load_wu = pltpu.make_async_copy(w_up, wgu.at[:, pl.ds(ff, ff)], w_sem.at[2])

    load_wd.start()
    for copy in load_block(0, 0):
        copy.start()
    load_wg.start()
    load_wu.start()

    barrier = pltpu.get_barrier_semaphore()
    for axis in (0, 1):
        for sign in (1, -1):
            pl.semaphore_signal(barrier, inc=1, device_id=device(axis, sign), device_id_type=MESH)
    pl.semaphore_wait(barrier, 4)

    def hop(h, c, b):
        a1, a2, sign = flows[c]
        slot = b % 2
        if h < HOPS:
            return pltpu.make_async_remote_copy(
                st1.at[h, c], rv1.at[slot, h, c], s1_send.at[h, c], r1_recv.at[slot, h, c],
                device_id=device(a1, sign), device_id_type=MESH,
            )
        if h < 2 * HOPS:
            s = h - HOPS
            return pltpu.make_async_remote_copy(
                st2.at[s, c], rv2.at[slot, s, c], s2_send.at[s, c], r2_recv.at[slot, s, c],
                device_id=device(a2, sign), device_id_type=MESH,
            )
        s = h - 2 * HOPS
        p1, p2 = pos[a1], pos[a2]
        if s < HOPS:
            q = (p2 + side - sign * s) % side
            r = pl.ds(pl.multiple_of(b * BLOCK + p1 * part + q * sub, sub), sub)
            to = device(a2, sign)
        else:
            q = (p1 + side - sign * (s - HOPS)) % side
            r = pl.ds(pl.multiple_of(b * BLOCK + q * part, part), part)
            to = device(a1, sign)
        where = dx.at[r, cols(c)]
        return pltpu.make_async_remote_copy(
            fin.at[c] if s == 0 else where, where, ag_send.at[s, c], ag_recv.at[slot, s, c],
            device_id=to, device_id_type=MESH,
        )

    def own_piece(c, b):
        a1, a2, sign = flows[c]
        r = pl.ds(pl.multiple_of(b * BLOCK + pos[a1] * part + pos[a2] * sub, sub), sub)
        return pltpu.make_async_copy(fin.at[c], dx.at[r, cols(c)], fin_sem.at[c])

    def term_part(b, c, q):
        r = pl.ds(pl.multiple_of(q * part, part), part)
        return term[b % 3, r, cols(c)]

    def stage(h, b, which=range(4)):
        for c in which:
            a1, a2, sign = flows[c]
            p1, p2 = pos[a1], pos[a2]
            if h > 0:
                hop(h - 1, c, b).wait_recv()
            if h < HOPS:
                q = (p1 + 2 * side - sign * (1 + h)) % side
                value = term_part(b, c, q)
                if h > 0:
                    value = value + rv1[b % 2, h - 1, c].astype(F32)
                st1[h, c] = value.astype(BF16)
            elif h < 2 * HOPS:
                s = h - HOPS
                if s == 0:
                    acc[b % 3, c] = term_part(b, c, p1) + rv1[b % 2, HOPS - 1, c].astype(F32)
                q = (p2 + 2 * side - sign * (1 + s)) % side
                value = acc[b % 3, c, pl.ds(pl.multiple_of(q * sub, sub), sub), :]
                if s > 0:
                    value = value + rv2[b % 2, s - 1, c].astype(F32)
                st2[s, c] = value.astype(BF16)
            elif h == 2 * HOPS:
                value = acc[b % 3, c, pl.ds(pl.multiple_of(p2 * sub, sub), sub), :]
                fin[c] = (value + rv2[b % 2, HOPS - 1, c].astype(F32)).astype(BF16)
                own_piece(c, b).start()
            elif h == 2 * HOPS + 1:
                own_piece(c, b).wait()
            if h < 4 * HOPS:
                hop(h, c, b).start()

    def front(t):
        slot = t % 2
        for copy in load_block(t, slot):
            copy.wait()

        @pl.when(t + 1 < blocks)
        def _():
            for copy in load_block(t + 1, 1 - slot):
                copy.start()

        @pl.when(t == 0)
        def _():
            load_wd.wait()

        dh[...] = lax.dot_general(dyb[slot], wd[...], LAST, preferred_element_type=F32)
        base = pl.multiple_of(t * BLOCK, BLOCK)

        @pl.loop(0, BLOCK // ACT_ROWS)
        def _(i):
            r = pl.ds(pl.multiple_of(i * ACT_ROWS, ACT_ROWS), ACT_ROWS)
            g = pl.ds(pl.multiple_of(base + i * ACT_ROWS, ACT_ROWS), ACT_ROWS)
            hidden, back = jax.vjp(act, gb[slot, r, :].astype(F32), ub[slot, r, :].astype(F32))
            d_gate, d_up = back(dh[r, :])
            dgu[g, pl.ds(0, ff)] = d_gate.astype(BF16)
            dgu[g, pl.ds(ff, ff)] = d_up.astype(BF16)
            hb[r, :] = hidden.astype(BF16)

        hid_t[:, pl.ds(base, BLOCK)] = hb[...].T

    def back_half(t, i):
        lhs = dgu[pl.ds(pl.multiple_of(t * BLOCK, BLOCK), BLOCK), :]
        n = pl.ds(i * (d // 2), d // 2)
        term[t % 3, :, n] = lax.dot_general(lhs, wgu[n, :], LAST, preferred_element_type=F32)

    def load_slab(j, slot):
        n = pl.ds(pl.multiple_of(j * SLAB, SLAB), SLAB)
        return (
            pltpu.make_async_copy(x.at[:, n], xb.at[slot], xy_sem.at[slot, 0]),
            pltpu.make_async_copy(dy.at[:, n], yb.at[slot], xy_sem.at[slot, 1]),
        )

    def weights(j):
        slot = j % 2
        for copy in load_slab(j, slot):
            copy.wait()

        n = pl.ds(pl.multiple_of(j * SLAB, SLAB), SLAB)
        xt[...] = xb[slot].T
        for i in range(2):
            f = pl.ds(i * ff, ff)
            wgu[n, f] = jnp.dot(xt[...], dgu[:, f], preferred_element_type=F32).astype(BF16)
        wd[:, n] = jnp.dot(hid_t[...], yb[slot], preferred_element_type=F32).astype(BF16)

        @pl.when(j + 2 < slabs)
        def _():
            for copy in load_slab(j + 2, slot):
                copy.start()

    @pl.loop(0, blocks + 4 * HOPS + 1)
    def _(t):
        def events(*hops):
            for h in hops:
                b = t - h
                if h < 4 * HOPS:
                    @pl.when((b >= 1) & (b <= blocks))
                    def _():
                        for c in range(4):
                            hop(h, c, b - 1).wait_send()

                if h > 0:
                    @pl.when((b >= 0) & (b < blocks))
                    def _():
                        stage(h, b)

        events(*range(4 * HOPS, 2, -1))

        @pl.when(t < blocks)
        def _():
            front(t)

        events(2)

        @pl.when(t == 0)
        def _():
            load_wg.wait()
            load_wu.wait()

        @pl.when(t < blocks)
        def _():
            back_half(t, 0)

        events(1, 0)

        @pl.when(t < blocks)
        def _():
            stage(0, t, (0, 1))
            back_half(t, 1)
            stage(0, t, (2, 3))

        @pl.when(t == blocks - 1)
        def _():
            for j in range(2):
                for copy in load_slab(j, j):
                    copy.start()

        first = (t - blocks) * 2

        @pl.when((t >= blocks) & (first < slabs))
        def _():
            @pl.loop(0, 2)
            def _(i):
                weights(first + i)


def finish(dx_in, wgu, wd, dx, dw_gate, dw_up, dw_down, buf, in_sem, out_sem, w_sem):
    ff = wd.shape[0]
    pieces = dx.shape[0] // BLOCK
    reads = []
    for i in range(pieces):
        r = pl.ds(i * BLOCK, BLOCK)
        copy = pltpu.make_async_copy(dx_in.at[r, :], buf.at[r, :], in_sem.at[i])
        copy.start()
        reads.append(copy)
    copies = [
        pltpu.make_async_copy(wgu.at[:, pl.ds(0, ff)], dw_gate, w_sem.at[0]),
        pltpu.make_async_copy(wgu.at[:, pl.ds(ff, ff)], dw_up, w_sem.at[1]),
        pltpu.make_async_copy(wd, dw_down, w_sem.at[2]),
    ]
    for copy in copies:
        copy.start()
    for i, read in enumerate(reads):
        r = pl.ds(i * BLOCK, BLOCK)
        read.wait()
        copy = pltpu.make_async_copy(buf.at[r, :], dx.at[r, :], out_sem.at[i])
        copy.start()
        copies.append(copy)
    for copy in copies:
        copy.wait()


def solution(mesh):
    n = mesh.shape["tp"]
    side = math.isqrt(n)

    def step(x, dy, gate, up, w_gate, w_up, w_down):
        rows, d = x.shape
        ff = w_down.shape[0]
        part = BLOCK // side
        sub = part // side
        quarter = d // 4
        hbm = pl.BlockSpec(memory_space=pl.ANY)
        dma = pltpu.SemaphoreType.DMA
        vmem = pl.BlockSpec(memory_space=pltpu.VMEM)
        dx_raw, dw_gu, dw_d = pl.pallas_call(
            functools.partial(kernel, side),
            out_shape=(
                pltpu.HBM((rows, d), BF16),
                pltpu.VMEM((d, 2 * ff), BF16),
                pltpu.VMEM((ff, d), BF16),
            ),
            in_specs=[hbm] * 7,
            out_specs=(hbm, vmem, vmem),
            scratch_shapes=[
                pltpu.VMEM((rows, 2 * ff), BF16),
                pltpu.VMEM((ff, rows), BF16),
                pltpu.VMEM((2, BLOCK, d), BF16),
                pltpu.VMEM((2, BLOCK, ff), BF16),
                pltpu.VMEM((2, BLOCK, ff), BF16),
                pltpu.VMEM((BLOCK, ff), F32),
                pltpu.VMEM((BLOCK, ff), BF16),
                pltpu.VMEM((3, BLOCK, d), F32),
                pltpu.VMEM((3, 4, part, quarter), F32),
                pltpu.VMEM((HOPS, 4, part, quarter), BF16),
                pltpu.VMEM((2, HOPS, 4, part, quarter), BF16),
                pltpu.VMEM((HOPS, 4, sub, quarter), BF16),
                pltpu.VMEM((2, HOPS, 4, sub, quarter), BF16),
                pltpu.VMEM((4, sub, quarter), BF16),
                pltpu.VMEM((2, rows, SLAB), BF16),
                pltpu.VMEM((SLAB, rows), BF16),
                pltpu.VMEM((2, rows, SLAB), BF16),
                dma((2, 3)),
                dma((3,)),
                dma((HOPS, 4)),
                dma((HOPS, 4)),
                dma((2, HOPS, 4)),
                dma((2, HOPS, 4)),
                dma((2 * HOPS, 4)),
                dma((2, 2 * HOPS, 4)),
                dma((4,)),
                dma((2, 2)),
            ],
            compiler_params=pltpu.CompilerParams(
                collective_id=0, has_side_effects=True, vmem_limit_bytes=47_000_000
            ),
        )(x, dy, gate, up, w_gate, w_up, w_down)
        pieces = rows // BLOCK
        return pl.pallas_call(
            finish,
            out_shape=(
                jax.ShapeDtypeStruct((rows, d), BF16),
                jax.ShapeDtypeStruct((d, ff), BF16),
                jax.ShapeDtypeStruct((d, ff), BF16),
                jax.ShapeDtypeStruct((ff, d), BF16),
            ),
            in_specs=[hbm, vmem, vmem],
            out_specs=(hbm,) * 4,
            scratch_shapes=[
                pltpu.VMEM((rows, d), BF16), dma((pieces,)), dma((pieces,)), dma((3,)),
            ],
            compiler_params=pltpu.CompilerParams(vmem_limit_bytes=20_000_000),
        )(
            pltpu.with_memory_space_constraint(dx_raw, pltpu.HBM),
            pltpu.with_memory_space_constraint(dw_gu, pltpu.VMEM),
            pltpu.with_memory_space_constraint(dw_d, pltpu.VMEM),
        )

    tokens, columns, rows = P("dp", None), P(None, "tp"), P("tp", None)
    return jax.shard_map(
        step,
        mesh=mesh,
        in_specs=(tokens, tokens, P("dp", "tp"), P("dp", "tp"), columns, columns, rows),
        out_specs=(tokens, P("dp", "tp"), P("dp", "tp"), P(("dp", "tp"), None)),
        check_vma=False,
    )
```

```python
import functools
import math

import jax
import jax.numpy as jnp
from jax import lax
from jax.experimental import pallas as pl
from jax.experimental.pallas import tpu as pltpu
from jax.sharding import PartitionSpec as P

MESH = pl.DeviceIdType.MESH
F32 = jnp.float32
BF16 = jnp.bfloat16
LAST = (((1,), (1,)), ((), ()))

BLOCK = 256
SLAB = 256
ACT_ROWS = 32
CHUNKS = 4
VMEM = 33_090_000
HOPS = 3


def act_back(gate, up, d_hidden):
    k = math.sqrt(2 / math.pi)
    square = gate * gate
    t = jnp.tanh(gate * (k + (k * 0.044715) * square))
    cdf = 0.5 + 0.5 * t
    gelu = gate * cdf
    slope = cdf + (0.5 * gate) * (1 - t * t) * (k + (3 * k * 0.044715) * square)
    return gelu * up, d_hidden * up * slope, d_hidden * gelu


def kernel(
    side, x, dy, gate, up, w_gate, w_up, w_down,
    dx, wgu, wd,
    dgu, hid_t, dh, term, acc, st1, rv1, st2, rv2, xb, xt, yb,
    in_sem, w_sem, s1_send, s2_send, r1_recv, r2_recv, ag_send, ag_recv, xy_sem, chunk_sem,
):
    rows, d = dx.shape
    ff = w_down.shape[0]
    blocks = rows // BLOCK
    part = BLOCK // side
    sub = part // side
    quarter = d // 4
    slabs = d // SLAB

    me = lax.axis_index("tp")
    px, py = me // side, me % side

    def device(axis, sign):
        if axis == 0:
            return {"tp": (px + side + sign) % side * side + py}
        return {"tp": px * side + (py + side + sign) % side}

    flows = ((0, 1, 1), (0, 1, -1), (1, 0, 1), (1, 0, -1))
    pos = (px, py)

    def cols(c):
        return pl.ds(c * quarter, quarter)

    def load_block(t):
        slot = t % 2
        r = pl.ds(pl.multiple_of(t * BLOCK, BLOCK), BLOCK)
        return (
            pltpu.make_async_copy(dy.at[r, :], dx.at[r, :], in_sem.at[slot, 0]),
            pltpu.make_async_copy(gate.at[r, :], dgu.at[r, pl.ds(0, ff)], in_sem.at[slot, 1]),
            pltpu.make_async_copy(up.at[r, :], dgu.at[r, pl.ds(ff, ff)], in_sem.at[slot, 2]),
        )

    def load_half(i):
        n = pl.ds(i * (d // 2), d // 2)
        return (
            pltpu.make_async_copy(w_gate.at[n, :], wgu.at[n, pl.ds(0, ff)], w_sem.at[i, 0]),
            pltpu.make_async_copy(w_up.at[n, :], wgu.at[n, pl.ds(ff, ff)], w_sem.at[i, 1]),
        )

    chunk = d // CHUNKS

    def load_chunk(i):
        n = pl.ds(i * chunk, chunk)
        return (
            pltpu.make_async_copy(w_down.at[:, n], wd.at[:, n], chunk_sem.at[i, 0]),
            pltpu.make_async_copy(dy.at[pl.ds(0, BLOCK), n], dx.at[pl.ds(0, BLOCK), n], chunk_sem.at[i, 1]),
        )

    for i in range(CHUNKS):
        for copy in load_chunk(i):
            copy.start()
    for copy in (*load_block(0)[1:], *load_half(0), *load_half(1)):
        copy.start()

    barrier = pltpu.get_barrier_semaphore()
    for axis in (0, 1):
        for sign in (1, -1):
            pl.semaphore_signal(barrier, inc=1, device_id=device(axis, sign), device_id_type=MESH)
    pl.semaphore_wait(barrier, 4)

    def hop(h, c, b):
        a1, a2, sign = flows[c]
        slot = b % 2
        if h < HOPS:
            return pltpu.make_async_remote_copy(
                st1.at[h, c], rv1.at[slot, h, c], s1_send.at[h, c], r1_recv.at[slot, h, c],
                device_id=device(a1, sign), device_id_type=MESH,
            )
        if h < 2 * HOPS:
            s = h - HOPS
            return pltpu.make_async_remote_copy(
                st2.at[s, c], rv2.at[slot, s, c], s2_send.at[s, c], r2_recv.at[slot, s, c],
                device_id=device(a2, sign), device_id_type=MESH,
            )
        s = h - 2 * HOPS
        p1, p2 = pos[a1], pos[a2]
        if s < HOPS:
            q = (p2 + side - sign * s) % side
            r = pl.ds(pl.multiple_of(b * BLOCK + p1 * part + q * sub, sub), sub)
            to = device(a2, sign)
        else:
            q = (p1 + side - sign * (s - HOPS)) % side
            r = pl.ds(pl.multiple_of(b * BLOCK + q * part, part), part)
            to = device(a1, sign)
        where = dx.at[r, cols(c)]
        return pltpu.make_async_remote_copy(
            where, where, ag_send.at[s, c], ag_recv.at[slot, s, c],
            device_id=to, device_id_type=MESH,
        )

    def term_part(b, c, q):
        r = pl.ds(pl.multiple_of(q * part, part), part)
        return term[b % 2, r, cols(c)]

    def stage(h, b, which=range(4)):
        for c in which:
            a1, a2, sign = flows[c]
            p1, p2 = pos[a1], pos[a2]
            if h > 0:
                hop(h - 1, c, b).wait_recv()
            if h < HOPS:
                q = (p1 + 2 * side - sign * (1 + h)) % side
                value = term_part(b, c, q)
                if h > 0:
                    value = value + rv1[b % 2, h - 1, c].astype(F32)
                st1[h, c] = value.astype(BF16)
                if h == HOPS - 1:
                    acc[b % 4, c] = term_part(b, c, p1)
            elif h < 2 * HOPS:
                s = h - HOPS
                if s == 0:
                    acc[b % 4, c] = acc[b % 4, c] + rv1[b % 2, HOPS - 1, c].astype(F32)
                q = (p2 + 2 * side - sign * (1 + s)) % side
                value = acc[b % 4, c, pl.ds(pl.multiple_of(q * sub, sub), sub), :]
                if s > 0:
                    value = value + rv2[b % 2, s - 1, c].astype(F32)
                st2[s, c] = value.astype(BF16)
            elif h == 2 * HOPS:
                value = acc[b % 4, c, pl.ds(pl.multiple_of(p2 * sub, sub), sub), :]
                r = pl.ds(pl.multiple_of(b * BLOCK + p1 * part + p2 * sub, sub), sub)
                dx[r, cols(c)] = (value + rv2[b % 2, HOPS - 1, c].astype(F32)).astype(BF16)
            if h < 4 * HOPS:
                hop(h, c, b).start()

    def front(t):
        base = pl.multiple_of(t * BLOCK, BLOCK)

        @pl.when(t == 0)
        def _():
            for i in range(CHUNKS):
                n = pl.ds(i * chunk, chunk)
                for copy in load_chunk(i):
                    copy.wait()
                value = lax.dot_general(
                    dx[pl.ds(0, BLOCK), n], wd[:, n], LAST, preferred_element_type=F32
                )
                dh[...] = value if i == 0 else dh[...] + value
            for copy in load_block(0)[1:]:
                copy.wait()

        @pl.when(t > 0)
        def _():
            for copy in load_block(t):
                copy.wait()
            dh[...] = lax.dot_general(
                dx[pl.ds(base, BLOCK), :], wd[...], LAST, preferred_element_type=F32
            )

        @pl.when(t + 1 < blocks)
        def _():
            for copy in load_block(t + 1):
                copy.start()

        @pl.loop(0, BLOCK // ACT_ROWS)
        def _(i):
            r = pl.ds(pl.multiple_of(i * ACT_ROWS, ACT_ROWS), ACT_ROWS)
            g = pl.ds(pl.multiple_of(base + i * ACT_ROWS, ACT_ROWS), ACT_ROWS)
            hidden, d_gate, d_up = act_back(
                dgu[g, pl.ds(0, ff)].astype(F32), dgu[g, pl.ds(ff, ff)].astype(F32), dh[r, :]
            )
            dgu[g, pl.ds(0, ff)] = d_gate.astype(BF16)
            dgu[g, pl.ds(ff, ff)] = d_up.astype(BF16)
            dx[g, pl.ds(0, ff)] = hidden.astype(BF16)

    def back_half(t, i):
        @pl.when(t == 0)
        def _():
            for copy in load_half(i):
                copy.wait()

        lhs = dgu[pl.ds(pl.multiple_of(t * BLOCK, BLOCK), BLOCK), :]
        n = pl.ds(i * (d // 2), d // 2)
        term[t % 2, :, n] = lax.dot_general(lhs, wgu[n, :], LAST, preferred_element_type=F32)

    def keep_hidden(t):
        r = pl.ds(pl.multiple_of(t * BLOCK, BLOCK), BLOCK)
        hid_t[:, r] = dx[r, pl.ds(0, ff)].T

    def load_x(j):
        n = pl.ds(pl.multiple_of(j * SLAB, SLAB), SLAB)
        return pltpu.make_async_copy(x.at[:, n], xb, xy_sem.at[0])

    def load_y(j):
        n = pl.ds(pl.multiple_of(j * SLAB, SLAB), SLAB)
        return pltpu.make_async_copy(dy.at[:, n], yb, xy_sem.at[1])

    def weights(j):
        n = pl.ds(pl.multiple_of(j * SLAB, SLAB), SLAB)
        load_x(j).wait()
        xt[...] = xb[...].T

        @pl.when(j + 1 < slabs)
        def _():
            load_x(j + 1).start()

        for i in range(2):
            f = pl.ds(i * ff, ff)
            wgu[n, f] = jnp.dot(xt[...], dgu[:, f], preferred_element_type=F32).astype(BF16)
        load_y(j).wait()
        wd[:, n] = jnp.dot(hid_t[...], yb[...], preferred_element_type=F32).astype(BF16)

        @pl.when(j + 1 < slabs)
        def _():
            load_y(j + 1).start()

    @pl.loop(0, blocks + 4 * HOPS + 1)
    def _(t):
        def events(*hops, which=range(4)):
            for h in hops:
                b = t - h
                if h < 4 * HOPS:
                    @pl.when((b >= 1) & (b <= blocks))
                    def _():
                        for c in which:
                            hop(h, c, b - 1).wait_send()

                if h > 0:
                    @pl.when((b >= 0) & (b < blocks))
                    def _():
                        stage(h, b, which)

        events(*range(4 * HOPS, 2, -1))

        @pl.when(t < blocks)
        def _():
            front(t)

        events(2)
        events(1, which=(0, 1))

        @pl.when(t < blocks)
        def _():
            back_half(t, 0)

        events(1, which=(2, 3))
        events(0)

        @pl.when(t < blocks)
        def _():
            stage(0, t, (0, 1))
            back_half(t, 1)
            keep_hidden(t)
            stage(0, t, (2, 3))

        @pl.when(t == blocks - 1)
        def _():
            load_x(0).start()
            load_y(0).start()

        first = (t - blocks) * 2

        @pl.when((t >= blocks) & (first < slabs))
        def _():
            @pl.loop(0, 2)
            def _(i):
                weights(first + i)


def finish(dx_in, wgu, wd, dx, dw_gate, dw_up, dw_down, sem):
    ff = wd.shape[0]
    copies = []

    def add(source, target, pieces):
        rows = target.shape[0] // pieces
        for i in range(pieces):
            r = pl.ds(i * rows, rows)
            copy = pltpu.make_async_copy(source(r), target.at[r, :], sem.at[len(copies)])
            copy.start()
            copies.append(copy)

    add(lambda r: dx_in.at[r, :], dx, 8)
    add(lambda r: wgu.at[r, pl.ds(0, ff)], dw_gate, 4)
    add(lambda r: wgu.at[r, pl.ds(ff, ff)], dw_up, 4)
    add(lambda r: wd.at[r, :], dw_down, 4)
    for copy in copies:
        copy.wait()


def solution(mesh):
    n = mesh.shape["tp"]
    side = math.isqrt(n)

    def step(x, dy, gate, up, w_gate, w_up, w_down):
        rows, d = x.shape
        ff = w_down.shape[0]
        part = BLOCK // side
        sub = part // side
        quarter = d // 4
        hbm = pl.BlockSpec(memory_space=pl.ANY)
        dma = pltpu.SemaphoreType.DMA
        vmem = pl.BlockSpec(memory_space=pltpu.VMEM)
        dx_raw, dw_gu, dw_d = pl.pallas_call(
            functools.partial(kernel, side),
            out_shape=(
                pltpu.VMEM((rows, d), BF16),
                pltpu.VMEM((d, 2 * ff), BF16),
                pltpu.VMEM((ff, d), BF16),
            ),
            in_specs=[hbm] * 7,
            out_specs=(vmem,) * 3,
            scratch_shapes=[
                pltpu.VMEM((rows, 2 * ff), BF16),
                pltpu.VMEM((ff, rows), BF16),
                pltpu.VMEM((BLOCK, ff), F32),
                pltpu.VMEM((2, BLOCK, d), F32),
                pltpu.VMEM((4, 4, part, quarter), F32),
                pltpu.VMEM((HOPS, 4, part, quarter), BF16),
                pltpu.VMEM((2, HOPS, 4, part, quarter), BF16),
                pltpu.VMEM((HOPS, 4, sub, quarter), BF16),
                pltpu.VMEM((2, HOPS, 4, sub, quarter), BF16),
                pltpu.VMEM((rows, SLAB), BF16),
                pltpu.VMEM((SLAB, rows), BF16),
                pltpu.VMEM((rows, SLAB), BF16),
                dma((2, 3)),
                dma((2, 2)),
                dma((HOPS, 4)),
                dma((HOPS, 4)),
                dma((2, HOPS, 4)),
                dma((2, HOPS, 4)),
                dma((2 * HOPS, 4)),
                dma((2, 2 * HOPS, 4)),
                dma((2,)),
                dma((CHUNKS, 2)),
            ],
            compiler_params=pltpu.CompilerParams(
                collective_id=0, has_side_effects=True, vmem_limit_bytes=VMEM
            ),
        )(x, dy, gate, up, w_gate, w_up, w_down)
        return pl.pallas_call(
            finish,
            out_shape=(
                jax.ShapeDtypeStruct((rows, d), BF16),
                jax.ShapeDtypeStruct((d, ff), BF16),
                jax.ShapeDtypeStruct((d, ff), BF16),
                jax.ShapeDtypeStruct((ff, d), BF16),
            ),
            in_specs=[vmem] * 3,
            out_specs=(hbm,) * 4,
            scratch_shapes=[dma((20,))],
            compiler_params=pltpu.CompilerParams(vmem_limit_bytes=VMEM),
        )(
            pltpu.with_memory_space_constraint(dx_raw, pltpu.VMEM),
            pltpu.with_memory_space_constraint(dw_gu, pltpu.VMEM),
            pltpu.with_memory_space_constraint(dw_d, pltpu.VMEM),
        )

    tokens, columns, rows = P("dp", None), P(None, "tp"), P("tp", None)
    return jax.shard_map(
        step,
        mesh=mesh,
        in_specs=(tokens, tokens, P("dp", "tp"), P("dp", "tp"), columns, columns, rows),
        out_specs=(tokens, P("dp", "tp"), P("dp", "tp"), P(("dp", "tp"), None)),
        check_vma=False,
    )
```

```python
import functools
import math

import jax
import jax.numpy as jnp
from jax import lax
from jax.experimental import pallas as pl
from jax.experimental.pallas import tpu as pltpu
from jax.sharding import PartitionSpec as P

MESH = pl.DeviceIdType.MESH
F32 = jnp.float32
BF16 = jnp.bfloat16
LAST = (((1,), (1,)), ((), ()))

BLOCK = 256
SLAB = 256
ACT_ROWS = 32
CHUNKS = 4
STARTS = (1, 3)
VMEM = 33_090_000
HOPS = 3


def act_back(gate, up, d_hidden):
    k = math.sqrt(2 / math.pi)
    square = gate * gate
    t = jnp.tanh(gate * (k + (k * 0.044715) * square))
    cdf = 0.5 + 0.5 * t
    gelu = gate * cdf
    slope = cdf + (0.5 * gate) * (1 - t * t) * (k + (3 * k * 0.044715) * square)
    return gelu * up, d_hidden * up * slope, d_hidden * gelu


def kernel(
    side, x, dy, gate, up, w_gate, w_up, w_down,
    dx, wgu, wd,
    dgu, hid_t, dh, term, acc, st1, rv1, st2, rv2, xb, xt, yb,
    in_sem, w_sem, s1_send, s2_send, r1_recv, r2_recv, ag_send, ag_recv, xy_sem, chunk_sem,
):
    rows, d = dx.shape
    ff = w_down.shape[0]
    blocks = rows // BLOCK
    part = BLOCK // side
    sub = part // side
    quarter = d // 4
    slabs = d // SLAB

    me = lax.axis_index("tp")
    px, py = me // side, me % side

    def device(axis, sign):
        if axis == 0:
            return {"tp": (px + side + sign) % side * side + py}
        return {"tp": px * side + (py + side + sign) % side}

    flows = ((0, 1, 1), (0, 1, -1), (1, 0, 1), (1, 0, -1))
    pos = (px, py)

    def cols(c):
        return pl.ds(c * quarter, quarter)

    def load_block(t):
        slot = t % 2
        r = pl.ds(pl.multiple_of(t * BLOCK, BLOCK), BLOCK)
        return (
            pltpu.make_async_copy(dy.at[r, :], dx.at[r, :], in_sem.at[slot, 0]),
            pltpu.make_async_copy(gate.at[r, :], dgu.at[r, pl.ds(0, ff)], in_sem.at[slot, 1]),
            pltpu.make_async_copy(up.at[r, :], dgu.at[r, pl.ds(ff, ff)], in_sem.at[slot, 2]),
        )

    def load_half(i):
        n = pl.ds(i * (d // 2), d // 2)
        return (
            pltpu.make_async_copy(w_gate.at[n, :], wgu.at[n, pl.ds(0, ff)], w_sem.at[i, 0]),
            pltpu.make_async_copy(w_up.at[n, :], wgu.at[n, pl.ds(ff, ff)], w_sem.at[i, 1]),
        )

    chunk = d // CHUNKS

    def load_chunk(i):
        n = pl.ds(i * chunk, chunk)
        return (
            pltpu.make_async_copy(w_down.at[:, n], wd.at[:, n], chunk_sem.at[i, 0]),
            pltpu.make_async_copy(dy.at[pl.ds(0, BLOCK), n], dx.at[pl.ds(0, BLOCK), n], chunk_sem.at[i, 1]),
        )

    for i in range(CHUNKS):
        for copy in load_chunk(i):
            copy.start()
    for copy in load_block(0)[1:]:
        copy.start()

    barrier = pltpu.get_barrier_semaphore()
    for axis in (0, 1):
        for sign in (1, -1):
            pl.semaphore_signal(barrier, inc=1, device_id=device(axis, sign), device_id_type=MESH)
    pl.semaphore_wait(barrier, 4)

    def hop(h, c, b):
        a1, a2, sign = flows[c]
        slot = b % 2
        if h < HOPS:
            return pltpu.make_async_remote_copy(
                st1.at[h, c], rv1.at[slot, h, c], s1_send.at[h, c], r1_recv.at[slot, h, c],
                device_id=device(a1, sign), device_id_type=MESH,
            )
        if h < 2 * HOPS:
            s = h - HOPS
            return pltpu.make_async_remote_copy(
                st2.at[s, c], rv2.at[slot, s, c], s2_send.at[s, c], r2_recv.at[slot, s, c],
                device_id=device(a2, sign), device_id_type=MESH,
            )
        s = h - 2 * HOPS
        p1, p2 = pos[a1], pos[a2]
        if s < HOPS:
            q = (p2 + side - sign * s) % side
            r = pl.ds(pl.multiple_of(b * BLOCK + p1 * part + q * sub, sub), sub)
            to = device(a2, sign)
        else:
            q = (p1 + side - sign * (s - HOPS)) % side
            r = pl.ds(pl.multiple_of(b * BLOCK + q * part, part), part)
            to = device(a1, sign)
        where = dx.at[r, cols(c)]
        return pltpu.make_async_remote_copy(
            where, where, ag_send.at[s, c], ag_recv.at[slot, s, c],
            device_id=to, device_id_type=MESH,
        )

    def term_part(b, c, q):
        r = pl.ds(pl.multiple_of(q * part, part), part)
        return term[b % 2, r, cols(c)]

    def stage(h, b, which=range(4)):
        for c in which:
            a1, a2, sign = flows[c]
            p1, p2 = pos[a1], pos[a2]
            if h > 0:
                hop(h - 1, c, b).wait_recv()
            if h < HOPS:
                q = (p1 + 2 * side - sign * (1 + h)) % side
                value = term_part(b, c, q)
                if h > 0:
                    value = value + rv1[b % 2, h - 1, c].astype(F32)
                st1[h, c] = value.astype(BF16)
                if h == HOPS - 1:
                    acc[b % 4, c] = term_part(b, c, p1)
            elif h < 2 * HOPS:
                s = h - HOPS
                if s == 0:
                    acc[b % 4, c] = acc[b % 4, c] + rv1[b % 2, HOPS - 1, c].astype(F32)
                q = (p2 + 2 * side - sign * (1 + s)) % side
                value = acc[b % 4, c, pl.ds(pl.multiple_of(q * sub, sub), sub), :]
                if s > 0:
                    value = value + rv2[b % 2, s - 1, c].astype(F32)
                st2[s, c] = value.astype(BF16)
            elif h == 2 * HOPS:
                value = acc[b % 4, c, pl.ds(pl.multiple_of(p2 * sub, sub), sub), :]
                r = pl.ds(pl.multiple_of(b * BLOCK + p1 * part + p2 * sub, sub), sub)
                dx[r, cols(c)] = (value + rv2[b % 2, HOPS - 1, c].astype(F32)).astype(BF16)
            if h < 4 * HOPS:
                hop(h, c, b).start()

    def front(t):
        base = pl.multiple_of(t * BLOCK, BLOCK)

        @pl.when(t == 0)
        def _():
            for i in range(CHUNKS):
                n = pl.ds(i * chunk, chunk)
                for copy in load_chunk(i):
                    copy.wait()
                if i in STARTS:
                    for copy in load_half(STARTS.index(i)):
                        copy.start()
                value = lax.dot_general(
                    dx[pl.ds(0, BLOCK), n], wd[:, n], LAST, preferred_element_type=F32
                )
                dh[...] = value if i == 0 else dh[...] + value
            for copy in load_block(0)[1:]:
                copy.wait()

        @pl.when(t > 0)
        def _():
            for copy in load_block(t):
                copy.wait()
            dh[...] = lax.dot_general(
                dx[pl.ds(base, BLOCK), :], wd[...], LAST, preferred_element_type=F32
            )

        @pl.when(t + 1 < blocks)
        def _():
            for copy in load_block(t + 1):
                copy.start()

        @pl.loop(0, BLOCK // ACT_ROWS)
        def _(i):
            r = pl.ds(pl.multiple_of(i * ACT_ROWS, ACT_ROWS), ACT_ROWS)
            g = pl.ds(pl.multiple_of(base + i * ACT_ROWS, ACT_ROWS), ACT_ROWS)
            hidden, d_gate, d_up = act_back(
                dgu[g, pl.ds(0, ff)].astype(F32), dgu[g, pl.ds(ff, ff)].astype(F32), dh[r, :]
            )
            dgu[g, pl.ds(0, ff)] = d_gate.astype(BF16)
            dgu[g, pl.ds(ff, ff)] = d_up.astype(BF16)
            dx[g, pl.ds(0, ff)] = hidden.astype(BF16)

    def back_half(t, i):
        @pl.when(t == 0)
        def _():
            for copy in load_half(i):
                copy.wait()

        lhs = dgu[pl.ds(pl.multiple_of(t * BLOCK, BLOCK), BLOCK), :]
        n = pl.ds(i * (d // 2), d // 2)
        term[t % 2, :, n] = lax.dot_general(lhs, wgu[n, :], LAST, preferred_element_type=F32)

    def keep_hidden(t):
        r = pl.ds(pl.multiple_of(t * BLOCK, BLOCK), BLOCK)
        hid_t[:, r] = dx[r, pl.ds(0, ff)].T

    def load_x(j):
        n = pl.ds(pl.multiple_of(j * SLAB, SLAB), SLAB)
        return pltpu.make_async_copy(x.at[:, n], xb, xy_sem.at[0])

    def load_y(j):
        n = pl.ds(pl.multiple_of(j * SLAB, SLAB), SLAB)
        return pltpu.make_async_copy(dy.at[:, n], yb, xy_sem.at[1])

    def weights(j):
        n = pl.ds(pl.multiple_of(j * SLAB, SLAB), SLAB)
        load_x(j).wait()
        xt[...] = xb[...].T

        @pl.when(j + 1 < slabs)
        def _():
            load_x(j + 1).start()

        for i in range(2):
            f = pl.ds(i * ff, ff)
            wgu[n, f] = jnp.dot(xt[...], dgu[:, f], preferred_element_type=F32).astype(BF16)
        load_y(j).wait()
        wd[:, n] = jnp.dot(hid_t[...], yb[...], preferred_element_type=F32).astype(BF16)

        @pl.when(j + 1 < slabs)
        def _():
            load_y(j + 1).start()

    @pl.loop(0, blocks + 4 * HOPS + 1)
    def _(t):
        def events(*hops, which=range(4)):
            for h in hops:
                b = t - h
                if h < 4 * HOPS:
                    @pl.when((b >= 1) & (b <= blocks))
                    def _():
                        for c in which:
                            hop(h, c, b - 1).wait_send()

                if h > 0:
                    @pl.when((b >= 0) & (b < blocks))
                    def _():
                        stage(h, b, which)

        events(*range(4 * HOPS, 3 * HOPS, -1))
        first = (t - blocks) * 2

        @pl.when((t >= blocks) & (first < slabs))
        def _():
            weights(first)

        events(*range(3 * HOPS, 2, -1))

        @pl.when(t < blocks)
        def _():
            front(t)

        events(2)
        events(1, which=(0, 1))

        @pl.when(t < blocks)
        def _():
            back_half(t, 0)

        events(1, which=(2, 3))
        events(0)

        @pl.when(t < blocks)
        def _():
            stage(0, t, (0, 1))
            back_half(t, 1)
            keep_hidden(t)
            stage(0, t, (2, 3))

        @pl.when(t == blocks - 1)
        def _():
            load_x(0).start()
            load_y(0).start()

        @pl.when((t >= blocks) & (first < slabs))
        def _():
            weights(first + 1)


def finish(dx_in, wgu, wd, dx, dw_gate, dw_up, dw_down, sem):
    ff = wd.shape[0]
    copies = []

    def add(source, target, pieces):
        rows = target.shape[0] // pieces
        for i in range(pieces):
            r = pl.ds(i * rows, rows)
            copy = pltpu.make_async_copy(source(r), target.at[r, :], sem.at[len(copies)])
            copy.start()
            copies.append(copy)

    add(lambda r: dx_in.at[r, :], dx, 8)
    add(lambda r: wgu.at[r, pl.ds(0, ff)], dw_gate, 4)
    add(lambda r: wgu.at[r, pl.ds(ff, ff)], dw_up, 4)
    add(lambda r: wd.at[r, :], dw_down, 4)
    for copy in copies:
        copy.wait()


def solution(mesh):
    n = mesh.shape["tp"]
    side = math.isqrt(n)

    def step(x, dy, gate, up, w_gate, w_up, w_down):
        rows, d = x.shape
        ff = w_down.shape[0]
        part = BLOCK // side
        sub = part // side
        quarter = d // 4
        hbm = pl.BlockSpec(memory_space=pl.ANY)
        dma = pltpu.SemaphoreType.DMA
        vmem = pl.BlockSpec(memory_space=pltpu.VMEM)
        dx_raw, dw_gu, dw_d = pl.pallas_call(
            functools.partial(kernel, side),
            out_shape=(
                pltpu.VMEM((rows, d), BF16),
                pltpu.VMEM((d, 2 * ff), BF16),
                pltpu.VMEM((ff, d), BF16),
            ),
            in_specs=[hbm] * 7,
            out_specs=(vmem,) * 3,
            scratch_shapes=[
                pltpu.VMEM((rows, 2 * ff), BF16),
                pltpu.VMEM((ff, rows), BF16),
                pltpu.VMEM((BLOCK, ff), F32),
                pltpu.VMEM((2, BLOCK, d), F32),
                pltpu.VMEM((4, 4, part, quarter), F32),
                pltpu.VMEM((HOPS, 4, part, quarter), BF16),
                pltpu.VMEM((2, HOPS, 4, part, quarter), BF16),
                pltpu.VMEM((HOPS, 4, sub, quarter), BF16),
                pltpu.VMEM((2, HOPS, 4, sub, quarter), BF16),
                pltpu.VMEM((rows, SLAB), BF16),
                pltpu.VMEM((SLAB, rows), BF16),
                pltpu.VMEM((rows, SLAB), BF16),
                dma((2, 3)),
                dma((2, 2)),
                dma((HOPS, 4)),
                dma((HOPS, 4)),
                dma((2, HOPS, 4)),
                dma((2, HOPS, 4)),
                dma((2 * HOPS, 4)),
                dma((2, 2 * HOPS, 4)),
                dma((2,)),
                dma((CHUNKS, 2)),
            ],
            compiler_params=pltpu.CompilerParams(
                collective_id=0, has_side_effects=True, vmem_limit_bytes=VMEM
            ),
        )(x, dy, gate, up, w_gate, w_up, w_down)
        return pl.pallas_call(
            finish,
            out_shape=(
                jax.ShapeDtypeStruct((rows, d), BF16),
                jax.ShapeDtypeStruct((d, ff), BF16),
                jax.ShapeDtypeStruct((d, ff), BF16),
                jax.ShapeDtypeStruct((ff, d), BF16),
            ),
            in_specs=[vmem] * 3,
            out_specs=(hbm,) * 4,
            scratch_shapes=[dma((20,))],
            compiler_params=pltpu.CompilerParams(vmem_limit_bytes=VMEM),
        )(
            pltpu.with_memory_space_constraint(dx_raw, pltpu.VMEM),
            pltpu.with_memory_space_constraint(dw_gu, pltpu.VMEM),
            pltpu.with_memory_space_constraint(dw_d, pltpu.VMEM),
        )

    tokens, columns, rows = P("dp", None), P(None, "tp"), P("tp", None)
    return jax.shard_map(
        step,
        mesh=mesh,
        in_specs=(tokens, tokens, P("dp", "tp"), P("dp", "tp"), columns, columns, rows),
        out_specs=(tokens, P("dp", "tp"), P("dp", "tp"), P(("dp", "tp"), None)),
        check_vma=False,
    )
```

```python
import functools
import math

import jax
import jax.numpy as jnp
from jax import lax
from jax.experimental import pallas as pl
from jax.experimental.pallas import tpu as pltpu
from jax.sharding import PartitionSpec as P

MESH = pl.DeviceIdType.MESH
F32 = jnp.float32
BF16 = jnp.bfloat16
LAST = (((1,), (1,)), ((), ()))

BLOCK = 256
SLAB = 256
ACT_ROWS = 32
CHUNKS = 4
STARTS = (1, 3)
VMEM = 33_090_000
RING = 3
SCATTER = 2
GATHER = SCATTER + RING
LAST_GATHER = GATHER + RING
ALL = LAST_GATHER + 2


def act_back(gate, up, d_hidden):
    k = math.sqrt(2 / math.pi)
    square = gate * gate
    t = jnp.tanh(gate * (k + (k * 0.044715) * square))
    cdf = 0.5 + 0.5 * t
    gelu = gate * cdf
    slope = cdf + (0.5 * gate) * (1 - t * t) * (k + (3 * k * 0.044715) * square)
    return gelu * up, d_hidden * up * slope, d_hidden * gelu


def kernel(
    side, x, dy, gate, up, w_gate, w_up, w_down,
    dx, wgu, wd,
    dgu, hid_t, dh, term, acc, st1, rv1, rvx, st2, rv2, xb, xt, yb,
    in_sem, w_sem, s1_send, s2_send, r1_recv, r2_recv, ag_send, ag_recv, xy_sem, chunk_sem,
):
    rows, d = dx.shape
    ff = w_down.shape[0]
    blocks = rows // BLOCK
    part = BLOCK // side
    sub = part // side
    quarter = d // 4
    slabs = d // SLAB

    me = lax.axis_index("tp")
    px, py = me // side, me % side

    def device(axis, sign):
        if axis == 0:
            return {"tp": (px + side + sign) % side * side + py}
        return {"tp": px * side + (py + side + sign) % side}

    flows = ((0, 1, 1), (0, 1, -1), (1, 0, 1), (1, 0, -1))
    pos = (px, py)

    def cols(c):
        return pl.ds(c * quarter, quarter)

    def load_block(t):
        slot = t % 2
        r = pl.ds(pl.multiple_of(t * BLOCK, BLOCK), BLOCK)
        return (
            pltpu.make_async_copy(dy.at[r, :], dx.at[r, :], in_sem.at[slot, 0]),
            pltpu.make_async_copy(gate.at[r, :], dgu.at[r, pl.ds(0, ff)], in_sem.at[slot, 1]),
            pltpu.make_async_copy(up.at[r, :], dgu.at[r, pl.ds(ff, ff)], in_sem.at[slot, 2]),
        )

    def load_half(i):
        n = pl.ds(i * (d // 2), d // 2)
        return (
            pltpu.make_async_copy(w_gate.at[n, :], wgu.at[n, pl.ds(0, ff)], w_sem.at[i, 0]),
            pltpu.make_async_copy(w_up.at[n, :], wgu.at[n, pl.ds(ff, ff)], w_sem.at[i, 1]),
        )

    chunk = d // CHUNKS

    def load_chunk(i):
        n = pl.ds(i * chunk, chunk)
        return (
            pltpu.make_async_copy(w_down.at[:, n], wd.at[:, n], chunk_sem.at[i, 0]),
            pltpu.make_async_copy(dy.at[pl.ds(0, BLOCK), n], dx.at[pl.ds(0, BLOCK), n], chunk_sem.at[i, 1]),
        )

    for i in range(CHUNKS):
        for copy in load_chunk(i):
            copy.start()
    for copy in load_block(0)[1:]:
        copy.start()

    barrier = pltpu.get_barrier_semaphore()
    for axis in (0, 1):
        for sign in (1, -1):
            pl.semaphore_signal(barrier, inc=1, device_id=device(axis, sign), device_id_type=MESH)
    pl.semaphore_wait(barrier, 4)

    def hop(h, c, b):
        a1, a2, sign = flows[c]
        slot = b % 2
        p1, p2 = pos[a1], pos[a2]
        if h < SCATTER:
            made = []
            for k in (0, 1) if h == 0 else (2,):
                late = b % 3 if k == 1 else slot
                made.append(pltpu.make_async_remote_copy(
                    st1.at[k, c], rvx.at[late, c] if k == 1 else rv1.at[slot, k // 2, c],
                    s1_send.at[k, c], r1_recv.at[late, k, c],
                    device_id=device(a1, sign), device_id_type=MESH,
                ))
            return made
        if h < GATHER:
            s = h - SCATTER
            return [pltpu.make_async_remote_copy(
                st2.at[s, c], rv2.at[slot, s, c], s2_send.at[s, c], r2_recv.at[slot, s, c],
                device_id=device(a2, sign), device_id_type=MESH,
            )]
        s = h - GATHER
        n = cols(c)
        if h < LAST_GATHER:
            q = (p2 + side - sign * s) % side
            r = pl.ds(pl.multiple_of(b * BLOCK + p1 * part + q * sub, sub), sub)
            to = device(a2, sign)
        else:
            q = p1
            if h == LAST_GATHER:
                n = pl.ds(c // 2 * 2 * quarter, 2 * quarter)
            else:
                q = (p1 + side - sign) % side
            r = pl.ds(pl.multiple_of(b * BLOCK + q * part, part), part)
            to = device(a1, sign)
        where = dx.at[r, n]
        return [pltpu.make_async_remote_copy(
            where, where, ag_send.at[s, c], ag_recv.at[slot, s, c],
            device_id=to, device_id_type=MESH,
        )]

    def term_part(b, c, q):
        r = pl.ds(pl.multiple_of(q * part, part), part)
        return term[b % 2, r, cols(c)]

    def stage(h, b, which=range(4)):
        if h in (SCATTER, LAST_GATHER):
            for c in which:
                hop(h - 1, c, b)[0].wait_recv()
                if h == SCATTER:
                    hop(0, c, b)[1].wait_recv()
        for c in which:
            a1, a2, sign = flows[c]
            p1, p2 = pos[a1], pos[a2]
            if h not in (0, SCATTER, LAST_GATHER):
                hop(h - 1, c, b)[0].wait_recv()
            near = (p1 + side + sign) % side
            if h == 0:
                st1[0, c] = term_part(b, c, (p1 + side + 2 * sign) % side).astype(BF16)
                st1[1, c] = term_part(b, c ^ 1, near).astype(BF16)
            elif h == 1:
                st1[2, c] = (term_part(b, c, near) + rv1[b % 2, 0, c].astype(F32)).astype(BF16)
            elif h < GATHER:
                s = h - SCATTER
                if s == 0:
                    acc[b % 3, c] = (
                        term_part(b, c, p1)
                        + rv1[b % 2, 1, c].astype(F32)
                        + rvx[b % 3, c ^ 1].astype(F32)
                    )
                q = (p2 + 2 * side - sign * (1 + s)) % side
                value = acc[b % 3, c, pl.ds(pl.multiple_of(q * sub, sub), sub), :]
                if s > 0:
                    value = value + rv2[b % 2, s - 1, c].astype(F32)
                st2[s, c] = value.astype(BF16)
            elif h == GATHER:
                value = acc[b % 3, c, pl.ds(pl.multiple_of(p2 * sub, sub), sub), :]
                r = pl.ds(pl.multiple_of(b * BLOCK + p1 * part + p2 * sub, sub), sub)
                dx[r, cols(c)] = (value + rv2[b % 2, RING - 1, c].astype(F32)).astype(BF16)
            if h < ALL:
                for copy in hop(h, c, b):
                    copy.start()

    def front(t):
        base = pl.multiple_of(t * BLOCK, BLOCK)

        @pl.when(t == 0)
        def _():
            for i in range(CHUNKS):
                n = pl.ds(i * chunk, chunk)
                for copy in load_chunk(i):
                    copy.wait()
                if i in STARTS:
                    for copy in load_half(STARTS.index(i)):
                        copy.start()
                value = lax.dot_general(
                    dx[pl.ds(0, BLOCK), n], wd[:, n], LAST, preferred_element_type=F32
                )
                dh[...] = value if i == 0 else dh[...] + value
            for copy in load_block(0)[1:]:
                copy.wait()

        @pl.when(t > 0)
        def _():
            for copy in load_block(t):
                copy.wait()
            dh[...] = lax.dot_general(
                dx[pl.ds(base, BLOCK), :], wd[...], LAST, preferred_element_type=F32
            )

        @pl.when(t + 1 < blocks)
        def _():
            for copy in load_block(t + 1):
                copy.start()

        @pl.loop(0, BLOCK // ACT_ROWS)
        def _(i):
            r = pl.ds(pl.multiple_of(i * ACT_ROWS, ACT_ROWS), ACT_ROWS)
            g = pl.ds(pl.multiple_of(base + i * ACT_ROWS, ACT_ROWS), ACT_ROWS)
            hidden, d_gate, d_up = act_back(
                dgu[g, pl.ds(0, ff)].astype(F32), dgu[g, pl.ds(ff, ff)].astype(F32), dh[r, :]
            )
            dgu[g, pl.ds(0, ff)] = d_gate.astype(BF16)
            dgu[g, pl.ds(ff, ff)] = d_up.astype(BF16)
            dx[g, pl.ds(0, ff)] = hidden.astype(BF16)

    def back_half(t, i):
        @pl.when(t == 0)
        def _():
            for copy in load_half(i):
                copy.wait()

        lhs = dgu[pl.ds(pl.multiple_of(t * BLOCK, BLOCK), BLOCK), :]
        n = pl.ds(i * (d // 2), d // 2)
        term[t % 2, :, n] = lax.dot_general(lhs, wgu[n, :], LAST, preferred_element_type=F32)

    def keep_hidden(t):
        r = pl.ds(pl.multiple_of(t * BLOCK, BLOCK), BLOCK)
        hid_t[:, r] = dx[r, pl.ds(0, ff)].T

    def load_x(j):
        n = pl.ds(pl.multiple_of(j * SLAB, SLAB), SLAB)
        return pltpu.make_async_copy(x.at[:, n], xb, xy_sem.at[0])

    def load_y(j):
        n = pl.ds(pl.multiple_of(j * SLAB, SLAB), SLAB)
        return pltpu.make_async_copy(dy.at[:, n], yb, xy_sem.at[1])

    def weights(j):
        n = pl.ds(pl.multiple_of(j * SLAB, SLAB), SLAB)
        load_x(j).wait()
        xt[...] = xb[...].T

        @pl.when(j + 1 < slabs)
        def _():
            load_x(j + 1).start()

        for i in range(2):
            f = pl.ds(i * ff, ff)
            wgu[n, f] = jnp.dot(xt[...], dgu[:, f], preferred_element_type=F32).astype(BF16)
        load_y(j).wait()
        wd[:, n] = jnp.dot(hid_t[...], yb[...], preferred_element_type=F32).astype(BF16)

        @pl.when(j + 1 < slabs)
        def _():
            load_y(j + 1).start()

    @pl.loop(0, blocks + ALL)
    def _(t):
        def events(*hops, which=range(4)):
            for h in hops:
                b = t - h
                if h < ALL:
                    @pl.when((b >= 1) & (b <= blocks))
                    def _():
                        for c in which:
                            for copy in hop(h, c, b - 1):
                                copy.wait_send()

                if h > 0:
                    @pl.when((b >= 0) & (b < blocks))
                    def _():
                        stage(h, b, which)

        events(*range(ALL, LAST_GATHER - 1, -1))
        first = (t - blocks) * 2

        @pl.when((t >= blocks) & (first < slabs))
        def _():
            weights(first)

        events(*range(LAST_GATHER - 1, SCATTER, -1))

        @pl.when(t < blocks)
        def _():
            front(t)

        events(SCATTER)
        events(1, which=(0, 1))

        @pl.when(t < blocks)
        def _():
            back_half(t, 0)

        events(1, which=(2, 3))
        events(0)

        @pl.when(t < blocks)
        def _():
            stage(0, t, (0, 1))
            back_half(t, 1)
            keep_hidden(t)
            stage(0, t, (2, 3))

        @pl.when(t == blocks - 1)
        def _():
            load_x(0).start()
            load_y(0).start()

        @pl.when((t >= blocks) & (first < slabs))
        def _():
            weights(first + 1)


def finish(dx_in, wgu, wd, dx, dw_gate, dw_up, dw_down, sem):
    ff = wd.shape[0]
    copies = []

    def add(source, target, pieces):
        rows = target.shape[0] // pieces
        for i in range(pieces):
            r = pl.ds(i * rows, rows)
            copy = pltpu.make_async_copy(source(r), target.at[r, :], sem.at[len(copies)])
            copy.start()
            copies.append(copy)

    add(lambda r: dx_in.at[r, :], dx, 8)
    add(lambda r: wgu.at[r, pl.ds(0, ff)], dw_gate, 4)
    add(lambda r: wgu.at[r, pl.ds(ff, ff)], dw_up, 4)
    add(lambda r: wd.at[r, :], dw_down, 4)
    for copy in copies:
        copy.wait()


def solution(mesh):
    n = mesh.shape["tp"]
    side = math.isqrt(n)

    def step(x, dy, gate, up, w_gate, w_up, w_down):
        rows, d = x.shape
        ff = w_down.shape[0]
        part = BLOCK // side
        sub = part // side
        quarter = d // 4
        hbm = pl.BlockSpec(memory_space=pl.ANY)
        dma = pltpu.SemaphoreType.DMA
        vmem = pl.BlockSpec(memory_space=pltpu.VMEM)
        dx_raw, dw_gu, dw_d = pl.pallas_call(
            functools.partial(kernel, side),
            out_shape=(
                pltpu.VMEM((rows, d), BF16),
                pltpu.VMEM((d, 2 * ff), BF16),
                pltpu.VMEM((ff, d), BF16),
            ),
            in_specs=[hbm] * 7,
            out_specs=(vmem,) * 3,
            scratch_shapes=[
                pltpu.VMEM((rows, 2 * ff), BF16),
                pltpu.VMEM((ff, rows), BF16),
                pltpu.VMEM((BLOCK, ff), F32),
                pltpu.VMEM((2, BLOCK, d), F32),
                pltpu.VMEM((3, 4, part, quarter), F32),
                pltpu.VMEM((3, 4, part, quarter), BF16),
                pltpu.VMEM((2, 2, 4, part, quarter), BF16),
                pltpu.VMEM((3, 4, part, quarter), BF16),
                pltpu.VMEM((RING, 4, sub, quarter), BF16),
                pltpu.VMEM((2, RING, 4, sub, quarter), BF16),
                pltpu.VMEM((rows, SLAB), BF16),
                pltpu.VMEM((SLAB, rows), BF16),
                pltpu.VMEM((rows, SLAB), BF16),
                dma((2, 3)),
                dma((2, 2)),
                dma((3, 4)),
                dma((RING, 4)),
                dma((3, 3, 4)),
                dma((2, RING, 4)),
                dma((RING + 2, 4)),
                dma((2, RING + 2, 4)),
                dma((2,)),
                dma((CHUNKS, 2)),
            ],
            compiler_params=pltpu.CompilerParams(
                collective_id=0, has_side_effects=True, vmem_limit_bytes=VMEM
            ),
        )(x, dy, gate, up, w_gate, w_up, w_down)
        return pl.pallas_call(
            finish,
            out_shape=(
                jax.ShapeDtypeStruct((rows, d), BF16),
                jax.ShapeDtypeStruct((d, ff), BF16),
                jax.ShapeDtypeStruct((d, ff), BF16),
                jax.ShapeDtypeStruct((ff, d), BF16),
            ),
            in_specs=[vmem] * 3,
            out_specs=(hbm,) * 4,
            scratch_shapes=[dma((20,))],
            compiler_params=pltpu.CompilerParams(vmem_limit_bytes=VMEM),
        )(
            pltpu.with_memory_space_constraint(dx_raw, pltpu.VMEM),
            pltpu.with_memory_space_constraint(dw_gu, pltpu.VMEM),
            pltpu.with_memory_space_constraint(dw_d, pltpu.VMEM),
        )

    tokens, columns, rows = P("dp", None), P(None, "tp"), P("tp", None)
    return jax.shard_map(
        step,
        mesh=mesh,
        in_specs=(tokens, tokens, P("dp", "tp"), P("dp", "tp"), columns, columns, rows),
        out_specs=(tokens, P("dp", "tp"), P("dp", "tp"), P(("dp", "tp"), None)),
        check_vma=False,
    )
```
